32 devices in a mesh: shard: 4 (over x, core), owner: 8 (over z, y).
Axes of the slice: x: 2, y: 2, z: 4, core: 2. Of those that a mesh axis runs over, the one named last changes fastest.
Arguments:
- gradient: float32 [32, 2048, 768], P('owner', 'shard'), may hold values from -6 to 6
- old_basis: float32 [32, 2048, 256], P('owner', 'shard'), may hold values from -0.125 to 0.125
- moment_one: float32 [32, 256, 768], P('owner', 'shard'), may hold values from -6 to 6
- moment_two: float32 [32, 256, 768], P('owner', 'shard'), may hold values from 0.01 to 1
- slot_expert: int32 [32], replicated, may hold values from 0 to 31, as said below
- cost: int32 [32], replicated, may hold values from 0 to 5
Outputs:
- new_basis: float32 [32, 2048, 256], P('owner', 'shard')
- new_moment_one: float32 [32, 256, 768], P('owner', 'shard')
- new_moment_two: float32 [32, 256, 768], P('owner', 'shard')
- update: bfloat16 [32, 2048, 768], P('owner', 'shard')
The draws below stay inside these ranges and needn't reach their ends.
Inputs may be any that keep to these rules, and one draw needn't show every extreme that they name: `slot_expert`: A permutation of the 32 experts. Expert e's gradient lies in owner group e // 4; state slot s lies in owner group s // 4. The 4 slots of one owner group hold experts of 4 different owner groups, and the 4 experts of one owner group are held by 4 different owner groups.
All inputs are finite; a program needn't handle non-finite values.
Results may differ from the reference program's by a relative error of at most 0.001.
Values sent between devices are 32-bit elements; how exact they have to be, the bound alone decides.
No kernel may reach another device: no remote copies, remote signals or barrier semaphores. Data moves between devices by JAX's collectives and lax.ppermute only.
A program may use at most 192 MiB of HBM per device.

```python
import math
import jax
import jax.numpy as jnp
from jax import lax

ROWS = 2048
COLS = 768
RANK = 256
ITERS = 5
SLOTS = 4
EXPERTS = 32


def joint_tables(key):
    owners = EXPERTS // SLOTS
    key_offset, key_homes, key_local, key_heavy, key_light = jax.random.split(jax.random.fold_in(key, 7), 5)
    offsets = jax.random.permutation(key_offset, owners)[:SLOTS].astype(jnp.int32)
    homes = jax.random.permutation(key_homes, owners).astype(jnp.int32)
    owner_ids = jnp.arange(owners, dtype=jnp.int32)
    home_of = homes[(owner_ids[:, None] + offsets[None, :]) % owners]
    local_perm = jax.vmap(lambda sub_key: jax.random.permutation(sub_key, SLOTS))(jax.random.split(key_local, owners)).astype(jnp.int32)
    slot_ids = jnp.arange(SLOTS, dtype=jnp.int32)
    local_index = local_perm[home_of, slot_ids[None, :]]
    slot_table = (home_of * SLOTS + local_index).reshape(-1).astype(jnp.int32)
    heavy = jax.random.randint(key_heavy, (owners,), 0, SLOTS, dtype=jnp.int32)
    light = jax.random.randint(key_light, (owners, SLOTS), 0, 2, dtype=jnp.int32)
    slot_cost = jnp.where(slot_ids[None, :] == heavy[:, None], ITERS, light).reshape(-1).astype(jnp.int32)
    cost_table = jnp.zeros((EXPERTS,), jnp.int32).at[slot_table].set(slot_cost)
    return (slot_table, cost_table)


def draw_slot_expert(key, part):
    return joint_tables(key)[0]


def draw_cost(key, part):
    return joint_tables(key)[1]


def block_scale(stream_key, extent, cuts, least, high):
    def one(dim, shards_of):
        draws = jax.random.uniform(jax.random.fold_in(jax.random.fold_in(stream_key, 6), dim), (shards_of,), jnp.float32, least / len(cuts), high / len(cuts))
        return jnp.repeat(jnp.exp(draws), extent[dim] // shards_of).reshape((-1,) + (1,) * (len(extent) - dim - 1))

    gain = one(*cuts[0])
    for cut in cuts[1:]:
        gain = gain * one(*cut)
    return gain


def bell_draw(stream_key, dims, scale, most, pieces=(), kind=jnp.bfloat16):
    array = jax.random.normal(stream_key, dims, jnp.float32) * scale
    if len(pieces) > 0:
        array = block_scale(stream_key, dims, pieces, -0.22, 0.18) * array
    return jnp.clip(array, min=-most, max=most).astype(kind)


def setup_inputs(seed: int = 0) -> dict:
    keys = jax.random.split(jax.random.key(seed), 7)
    return {
        "gradient": bell_draw(keys[0], (EXPERTS, ROWS, COLS), 1.0, 6.0, ((0, 8), (1, 4)), jnp.float32),
        "old_basis": bell_draw(keys[1], (EXPERTS, ROWS, RANK), ROWS ** -0.5, 0.125, ((0, 8), (1, 4)), jnp.float32),
        "moment_one": bell_draw(keys[2], (EXPERTS, RANK, COLS), 1.0, 6.0, ((0, 8), (1, 4)), jnp.float32),
        "moment_two": jnp.clip(jnp.exp(math.log(1.0) - 4.6051702 * jax.random.uniform(keys[3], (EXPERTS, RANK, COLS), jnp.float32) ** block_scale(keys[3], (EXPERTS, RANK, COLS), ((0, 8), (1, 4)), -0.2, 0.2)), 0.01, 1.0),
        "slot_expert": draw_slot_expert(jax.random.fold_in(keys[6], 71), 0),
        "cost": draw_cost(jax.random.fold_in(keys[6], 71), 0),
    }


HIGHEST_PREC = lax.Precision.HIGHEST
BETA_ONE = 0.9
BETA_TWO = 0.99
EPSILON = 1e-08
GALORE_SCALE = 0.25

def whole_step(basis_now, grad_now):
    inner_prod = jnp.dot(grad_now.T, basis_now, precision=HIGHEST_PREC)
    tall_block = jnp.dot(grad_now, inner_prod, precision=HIGHEST_PREC)
    gram_matrix = jnp.dot(tall_block.T, tall_block, precision=HIGHEST_PREC)
    factor = jnp.linalg.cholesky(gram_matrix)
    return lax.linalg.triangular_solve(factor, tall_block, left_side=False, lower=True, transpose_a=True)

def refresh(grad_now, basis_now, iter_count):
    return lax.fori_loop(0, iter_count, lambda step_index, current: whole_step(current, grad_now), basis_now)

def reference(gradient, old_basis, moment_one, moment_two, slot_expert, cost):

    def per_slot(slot_index):
        expert = slot_expert[slot_index]
        grad_now = gradient[expert]
        basis_new = refresh(grad_now, old_basis[slot_index], cost[expert])
        projected = jnp.dot(basis_new.T, grad_now, precision=HIGHEST_PREC)
        moment_new = BETA_ONE * moment_one[slot_index] + (1.0 - BETA_ONE) * projected
        second_new = BETA_TWO * moment_two[slot_index] + (1.0 - BETA_TWO) * projected * projected
        normed = moment_new / (jnp.sqrt(second_new) + EPSILON)
        update = (GALORE_SCALE * jnp.dot(basis_new, normed, precision=HIGHEST_PREC)).astype(jnp.bfloat16)
        return (basis_new, moment_new, second_new, update)
    basis_all, moment_all, second_all, update_all = lax.map(per_slot, jnp.arange(EXPERTS, dtype=jnp.int32))
    return (basis_all, moment_all, second_all, update_all)
```

```python
import functools

import jax
import jax.numpy as jnp
from jax import lax
from jax.experimental import pallas as pl
from jax.experimental.pallas import tpu as pltpu
from jax.sharding import PartitionSpec as P

HIGHEST_PREC = lax.Precision.HIGHEST
BETA_ONE = 0.9
BETA_TWO = 0.99
EPSILON = 1e-08
GALORE_SCALE = 0.25
LANES = 128
SUBS = 8


def dot_nn(a, b):
    return lax.dot_general(
        a, b, (((1,), (0,)), ((), ())), precision=HIGHEST_PREC, preferred_element_type=jnp.float32
    )


def dot_nt(a, b):
    return lax.dot_general(
        a, b, (((1,), (1,)), ((), ())), precision=HIGHEST_PREC, preferred_element_type=jnp.float32
    )


def chol_inverse_tile(block):
    width = block.shape[1]
    rows = [block[i * SUBS : (i + 1) * SUBS, :] for i in range(width // SUBS)]
    lane = lax.broadcasted_iota(jnp.int32, (SUBS, width), 1)
    sub = lax.broadcasted_iota(jnp.int32, (SUBS, width), 0)
    full = (SUBS, width)
    done = []
    for j in range(len(rows)):
        base = j * SUBS
        now = rows[j]
        in_block = (lane >= base) & (lane < base + SUBS)
        cols = [
            jnp.broadcast_to(now[:, base + p : base + p + 1], full) for p in range(SUBS)
        ]
        now = jnp.where(in_block, jnp.where(lane - base == sub, 1.0, 0.0), now)
        out = jnp.zeros(full, jnp.float32)
        for p in range(SUBS):
            pivot = jnp.broadcast_to(cols[p][p : p + 1, :], full)
            root = lax.rsqrt(pivot)
            inverse = root * root
            scaled = cols[p] * inverse
            line = jnp.broadcast_to(now[p : p + 1, :], full)
            out = jnp.where(sub == p, line * root, out)
            now = jnp.where(sub == p, line * inverse, now - scaled * line)
            for q in range(p + 1, SUBS):
                head = jnp.broadcast_to(cols[q][p : p + 1, :], full)
                cols[q] = jnp.where(sub == p, head * inverse, cols[q] - scaled * head)
        lines = [jnp.broadcast_to(now[p : p + 1, :], full) for p in range(SUBS)]
        for i in range(j + 1, len(rows)):
            terms = [
                jnp.broadcast_to(rows[i][:, base + p : base + p + 1], full) * lines[p]
                for p in range(SUBS)
            ]
            while len(terms) > 1:
                terms = [terms[k] + terms[k + 1] for k in range(0, len(terms), 2)]
            rows[i] = jnp.where(in_block, 0.0, rows[i]) - terms[0]
        done.append(jnp.where(lane <= base + sub, out, 0.0))
    return jnp.concatenate(done, axis=0)


def chol_inverse(gram_ref, out_ref):
    half = LANES
    first = chol_inverse_tile(gram_ref[:half, :half])
    out_ref[:half, :half] = first
    out_ref[:half, half:] = jnp.zeros((half, half), jnp.float32)
    low = dot_nt(gram_ref[half:, :half], first)
    second = chol_inverse_tile(gram_ref[half:, half:] - dot_nt(low, low))
    out_ref[half:, half:] = second
    out_ref[half:, :half] = -dot_nn(second, dot_nn(low, first))


def refine_kernel(count_ref, square_ref, start_ref, head_ref, state_ref, wide_ref, gram_ref, inv_ref):
    state_ref[...] = start_ref[...]
    head_ref[...] = jnp.zeros_like(head_ref)

    def step(_, carry):
        wide_ref[...] = dot_nn(state_ref[...], square_ref[...])
        gram_ref[...] = dot_nt(state_ref[...], wide_ref[...])
        chol_inverse(gram_ref, inv_ref)
        head_ref[...] = dot_nn(inv_ref[...], state_ref[...])
        state_ref[...] = dot_nn(inv_ref[...], wide_ref[...])
        return carry

    lax.fori_loop(0, count_ref[0], step, 0)


def refine(count, square, start):
    rank, cols = start.shape
    vmem = pl.BlockSpec(memory_space=pltpu.VMEM)
    shape = jax.ShapeDtypeStruct((rank, cols), jnp.float32)
    return pl.pallas_call(
        refine_kernel,
        out_shape=(shape, shape),
        in_specs=[pl.BlockSpec(memory_space=pltpu.SMEM), vmem, vmem],
        out_specs=(vmem, vmem),
        scratch_shapes=[
            pltpu.VMEM((rank, cols), jnp.float32),
            pltpu.VMEM((rank, rank), jnp.float32),
            pltpu.VMEM((rank, rank), jnp.float32),
        ],
        cost_estimate=pl.CostEstimate(
            flops=10 * rank * cols * cols, bytes_accessed=4 * cols * (cols + 3 * rank), transcendentals=0
        ),
        name="refine",
    )(count, square, start)


def pick(stack, index):
    return lax.dynamic_index_in_dim(stack, index, 0, keepdims=False)


def shard_shift(block_of, shift):
    size = lax.axis_size("shard")
    me = lax.axis_index("shard")
    block = block_of(lax.rem(me + shift, size))
    if shift == 0:
        return block
    return lax.ppermute(block, "shard", [(s, (s + shift) % size) for s in range(size)])


def shard_exchange(block_of):
    size = lax.axis_size("shard")
    me = lax.axis_index("shard")
    arrived = [shard_shift(block_of, shift) for shift in range(size)]
    stack = jnp.zeros((size,) + arrived[0].shape, arrived[0].dtype)
    for shift in range(size):
        stack = lax.dynamic_update_index_in_dim(
            stack, arrived[shift], lax.rem(me - shift + size, size), 0
        )
    return stack


def owner_exchange(stack):
    return lax.all_to_all(stack, "owner", split_axis=0, concat_axis=0, tiled=True)


def on_device(gradient, old_basis, moment_one, moment_two, slot_expert, cost):
    slots, rows, cols = gradient.shape
    rank = old_basis.shape[2]
    owners = lax.axis_size("owner")
    owner_now = lax.axis_index("owner")
    shard_now = lax.axis_index("shard")
    table = slot_expert.reshape(owners, slots)
    mine = lax.dynamic_index_in_dim(table, owner_now, 0, keepdims=False)
    home_of = mine // slots
    group = jnp.arange(owners)
    place = jnp.arange(slots)
    slot_for = jnp.sum(jnp.where(home_of[None, :] == group[:, None], place[None, :], 0), axis=1)
    hits = table[:, :, None] == (owner_now * slots + place)[None, None, :]
    local_for = jnp.sum(jnp.where(jnp.any(hits, axis=1), place[None, :], 0), axis=1)
    holder_of = jnp.sum(jnp.where(jnp.any(hits, axis=1), group[:, None], 0), axis=0)
    count = lax.dynamic_slice_in_dim(cost, owner_now * slots + shard_now, 1)

    outgoing = jnp.stack([pick(old_basis, slot_for[h]) for h in range(owners)])
    grad_now = shard_exchange(lambda i: pick(gradient, i)).reshape(-1, cols)
    arrived = owner_exchange(outgoing)
    basis_now = shard_exchange(lambda i: pick(arrived, pick(holder_of, i))).reshape(-1, rank)

    square = jnp.dot(grad_now.T, grad_now, precision=HIGHEST_PREC)
    start = jnp.dot(basis_now.T, grad_now, precision=HIGHEST_PREC)
    head, projected = refine(count, square, start)
    refreshed = lax.dot_general(
        grad_now, head, (((1,), (1,)), ((), ())), precision=HIGHEST_PREC
    )
    basis_new = jnp.where(count[0] > 0, refreshed, basis_now)

    part = projected.reshape(slots, -1, cols)
    proj_home = shard_exchange(lambda i: pick(part, i))
    proj_recv = owner_exchange(jnp.stack([pick(proj_home, local_for[o]) for o in range(owners)]))
    proj_slot = jnp.stack([pick(proj_recv, home_of[j]) for j in range(slots)])
    moment_new = BETA_ONE * moment_one + (1.0 - BETA_ONE) * proj_slot
    second_new = BETA_TWO * moment_two + (1.0 - BETA_TWO) * proj_slot * proj_slot
    normed = moment_new / (jnp.sqrt(second_new) + EPSILON)
    normed_all = lax.all_gather(normed, "shard", axis=1, tiled=True)

    block = basis_new.reshape(slots, rows, rank)
    basis_home = shard_exchange(lambda i: pick(block, i))
    basis_recv = owner_exchange(jnp.stack([pick(basis_home, local_for[o]) for o in range(owners)]))
    basis_slot = jnp.stack([pick(basis_recv, home_of[j]) for j in range(slots)])

    expanded = jnp.einsum("krq,kqc->krc", basis_slot, normed_all, precision=HIGHEST_PREC)
    update = (GALORE_SCALE * expanded).astype(jnp.bfloat16)
    return (basis_slot, moment_new, second_new, update)


def solution(mesh):
    spec = P("owner", "shard", None)
    return jax.shard_map(
        on_device,
        mesh=mesh,
        in_specs=(spec, spec, spec, spec, P(), P()),
        out_specs=(spec, spec, spec, spec),
        check_vma=False,
    )
```

```python
import functools

import jax
import jax.numpy as jnp
from jax import lax
from jax.experimental import pallas as pl
from jax.experimental.pallas import tpu as pltpu
from jax.sharding import PartitionSpec as P

HIGHEST_PREC = lax.Precision.HIGHEST
HIGH_PREC = lax.Precision.HIGH
BETA_ONE = 0.9
BETA_TWO = 0.99
EPSILON = 1e-08
GALORE_SCALE = 0.25
SUBS = 8


def dot_nn(a, b):
    return lax.dot_general(
        a, b, (((1,), (0,)), ((), ())), precision=HIGHEST_PREC, preferred_element_type=jnp.float32
    )


def dot_nt(a, b):
    return lax.dot_general(
        a, b, (((1,), (1,)), ((), ())), precision=HIGHEST_PREC, preferred_element_type=jnp.float32
    )


def chol_inverse_tile(block):
    width = block.shape[1]
    rows = [block[i * SUBS : (i + 1) * SUBS, :] for i in range(width // SUBS)]
    lane = lax.broadcasted_iota(jnp.int32, (SUBS, width), 1)
    sub = lax.broadcasted_iota(jnp.int32, (SUBS, width), 0)
    full = (SUBS, width)
    done = []
    for j in range(len(rows)):
        base = j * SUBS
        now = rows[j]
        in_block = (lane >= base) & (lane < base + SUBS)
        cols = [
            jnp.where(lane >= 0, jnp.broadcast_to(now[:, base + p : base + p + 1], full), 0.0)
            for p in range(SUBS)
        ]
        now = jnp.where(in_block, jnp.where(lane - base == sub, 1.0, 0.0), now)
        out = jnp.zeros(full, jnp.float32)
        for p in range(SUBS):
            pivot = jnp.broadcast_to(cols[p][p : p + 1, :], full)
            root = lax.rsqrt(pivot)
            inverse = root * root
            scaled = cols[p] * inverse
            line = jnp.broadcast_to(now[p : p + 1, :], full)
            out = jnp.where(sub == p, line * root, out)
            now = jnp.where(sub == p, line * inverse, now - scaled * line)
            for q in range(p + 1, SUBS):
                head = jnp.broadcast_to(cols[q][p : p + 1, :], full)
                cols[q] = jnp.where(sub == p, head * inverse, cols[q] - scaled * head)
        lines = [jnp.broadcast_to(now[p : p + 1, :], full) for p in range(SUBS)]
        for i in range(j + 1, len(rows)):
            terms = [
                jnp.broadcast_to(rows[i][:, base + p : base + p + 1], full) * lines[p]
                for p in range(SUBS)
            ]
            while len(terms) > 1:
                terms = [terms[k] + terms[k + 1] for k in range(0, len(terms), 2)]
            rows[i] = jnp.where(in_block, 0.0, rows[i]) - terms[0]
        done.append(jnp.where(lane <= base + sub, out, 0.0))
    return jnp.concatenate(done, axis=0)


def chol_inverse(gram_ref, out_ref):
    half = gram_ref.shape[0] // 2
    first = chol_inverse_tile(gram_ref[:half, :half])
    out_ref[:half, :half] = first
    out_ref[:half, half:] = jnp.zeros((half, half), jnp.float32)
    low = dot_nt(gram_ref[half:, :half], first)
    second = chol_inverse_tile(gram_ref[half:, half:] - dot_nt(low, low))
    out_ref[half:, half:] = second
    out_ref[half:, :half] = -dot_nn(second, dot_nn(low, first))


def split(x):
    high = x.astype(jnp.bfloat16)
    return high, (x - high.astype(jnp.float32)).astype(jnp.bfloat16)


def dot_split(a, b, contract):
    def one(x, y):
        return lax.dot_general(
            x, y, (contract, ((), ())), preferred_element_type=jnp.float32
        )

    return one(a[0], b[1]) + one(a[1], b[0]) + one(a[0], b[0])


NN = ((1,), (0,))
NT = ((1,), (1,))


def refine_kernel(
    count_ref, square_ref, start_ref, head_ref, state_ref, square_parts, state_parts, wide_parts, gram_ref, inv_ref
):
    count = count_ref[0]
    state_ref[...] = start_ref[...]
    head_ref[...] = jnp.zeros_like(head_ref)
    square_parts[0], square_parts[1] = split(square_ref[...])
    state_parts[0], state_parts[1] = split(start_ref[...])

    def step(index, carry):
        state = (state_parts[0], state_parts[1])
        wide = split(dot_split(state, (square_parts[0], square_parts[1]), NN))
        wide_parts[0], wide_parts[1] = wide
        gram_ref[...] = dot_split(state, wide, NT)
        chol_inverse(gram_ref, inv_ref)
        inverse = split(inv_ref[...])

        @pl.when(index == count - 1)
        def _():
            head_ref[...] = dot_split(inverse, (state_parts[0], state_parts[1]), NN)

        fresh = dot_split(inverse, (wide_parts[0], wide_parts[1]), NN)
        state_ref[...] = fresh
        state_parts[0], state_parts[1] = split(fresh)
        return carry

    lax.fori_loop(0, count, step, 0)


def refine(count, square, start):
    rank, cols = start.shape
    vmem = pl.BlockSpec(memory_space=pltpu.VMEM)
    shape = jax.ShapeDtypeStruct((rank, cols), jnp.float32)
    return pl.pallas_call(
        refine_kernel,
        out_shape=(shape, shape),
        in_specs=[pl.BlockSpec(memory_space=pltpu.SMEM), vmem, vmem],
        out_specs=(vmem, vmem),
        scratch_shapes=[
            pltpu.VMEM((2, cols, cols), jnp.bfloat16),
            pltpu.VMEM((2, rank, cols), jnp.bfloat16),
            pltpu.VMEM((2, rank, cols), jnp.bfloat16),
            pltpu.VMEM((rank, rank), jnp.float32),
            pltpu.VMEM((rank, rank), jnp.float32),
        ],
        cost_estimate=pl.CostEstimate(
            flops=10 * rank * cols * cols, bytes_accessed=4 * cols * (cols + 3 * rank), transcendentals=0
        ),
        name="refine",
    )(count, square, start)


class Places:
    def __init__(self, owners, slots):
        self.owners, self.slots = owners, slots

    def home_of(self, slot, ids, table):
        return lax.div(table[ids[0] * self.slots + slot], self.slots)

    def slot_for(self, home, ids, table):
        found = 0
        for slot in range(self.slots):
            found = jnp.where(self.home_of(slot, ids, table) == home, slot, found)
        return found

    def local_for(self, holder, ids, table):
        found = 0
        for slot in range(self.slots):
            expert = table[holder * self.slots + slot]
            hit = lax.div(expert, self.slots) == ids[0]
            found = jnp.where(hit, lax.rem(expert, self.slots), found)
        return found

    def holder_of(self, local, ids, table):
        wanted = ids[0] * self.slots + local
        found = 0
        for entry in range(self.owners * self.slots):
            found = jnp.where(table[entry] == wanted, entry // self.slots, found)
        return found


def copy_block(ids_ref, table_ref, in_ref, out_ref):
    out_ref[...] = in_ref[...]


def pick_stack(ids, table, stack, number, index):
    block = (1,) + stack.shape[1:]
    return pl.pallas_call(
        copy_block,
        out_shape=jax.ShapeDtypeStruct((number,) + stack.shape[1:], stack.dtype),
        grid_spec=pltpu.PrefetchScalarGridSpec(
            num_scalar_prefetch=2,
            grid=(number,),
            in_specs=[pl.BlockSpec(block, lambda n, i, t: (index(n, i, t), 0, 0))],
            out_specs=pl.BlockSpec(block, lambda n, i, t: (n, 0, 0)),
        ),
        name="pick_stack",
    )(ids, table, stack)


def copy_apart(number, ids_ref, table_ref, *refs):
    for k in range(number):
        refs[number + k][...] = refs[k][0]


def pick_apart(ids, table, stack, number, index, steps=2):
    _, rows, cols = stack.shape
    part = rows // steps

    def source(k):
        return pl.BlockSpec((1, part, cols), lambda r, i, t: (index(k, i, t), r, 0))

    return pl.pallas_call(
        functools.partial(copy_apart, number),
        out_shape=[jax.ShapeDtypeStruct((rows, cols), stack.dtype)] * number,
        grid_spec=pltpu.PrefetchScalarGridSpec(
            num_scalar_prefetch=2,
            grid=(steps,),
            in_specs=[source(k) for k in range(number)],
            out_specs=[pl.BlockSpec((part, cols), lambda r, i, t: (r, 0))] * number,
        ),
        name="pick_apart",
    )(ids, table, *([stack] * number))


def choose_block(places, number, ids_ref, table_ref, *refs):
    out_ref = refs[number]
    for holder in range(places.owners):
        local = places.local_for(holder, ids_ref, table_ref)
        shift = lax.rem(local - ids_ref[1] + number, number)
        for k in range(number):

            @pl.when(shift == k)
            def _():
                out_ref[holder] = refs[k][...]


def stack_for_holders(places, ids, table, blocks, steps):
    rows, cols = blocks[0].shape
    part = rows // steps
    return pl.pallas_call(
        functools.partial(choose_block, places, len(blocks)),
        out_shape=jax.ShapeDtypeStruct((places.owners, rows, cols), blocks[0].dtype),
        grid_spec=pltpu.PrefetchScalarGridSpec(
            num_scalar_prefetch=2,
            grid=(steps,),
            in_specs=[pl.BlockSpec((part, cols), lambda r, i, t: (r, 0))] * len(blocks),
            out_specs=pl.BlockSpec((places.owners, part, cols), lambda r, i, t: (0, r, 0)),
        ),
        name="stack_for_holders",
    )(ids, table, *blocks)


def adam_kernel(ids_ref, table_ref, proj_ref, one_ref, two_ref, one_out, two_out, normed_ref):
    projected = proj_ref[...]
    moment_new = BETA_ONE * one_ref[...] + (1.0 - BETA_ONE) * projected
    second_new = BETA_TWO * two_ref[...] + (1.0 - BETA_TWO) * projected * projected
    one_out[...] = moment_new
    two_out[...] = second_new
    normed_ref[...] = moment_new / (jnp.sqrt(second_new) + EPSILON)


def adam(places, ids, table, received, moment_one, moment_two):
    block = (1,) + moment_one.shape[1:]
    own = pl.BlockSpec(block, lambda n, i, t: (n, 0, 0))
    shape = jax.ShapeDtypeStruct(moment_one.shape, moment_one.dtype)
    return pl.pallas_call(
        adam_kernel,
        out_shape=[shape] * 3,
        grid_spec=pltpu.PrefetchScalarGridSpec(
            num_scalar_prefetch=2,
            grid=(moment_one.shape[0],),
            in_specs=[
                pl.BlockSpec(block, lambda n, i, t: (places.home_of(n, i, t), 0, 0)),
                own,
                own,
            ],
            out_specs=[own] * 3,
        ),
        name="adam",
    )(ids, table, received, moment_one, moment_two)


def update_kernel(ids_ref, table_ref, basis_ref, normed_ref, basis_out, update_ref):
    basis = basis_ref[0]
    basis_out[0] = basis
    expanded = dot_split(split(basis), split(normed_ref[0]), NN)
    update_ref[0] = (GALORE_SCALE * expanded).astype(update_ref.dtype)


def updates(places, ids, table, received, normed, slots):
    _, rows, rank = received.shape
    cols = normed.shape[2]
    return pl.pallas_call(
        update_kernel,
        out_shape=[
            jax.ShapeDtypeStruct((slots, rows, rank), jnp.float32),
            jax.ShapeDtypeStruct((slots, rows, cols), jnp.bfloat16),
        ],
        grid_spec=pltpu.PrefetchScalarGridSpec(
            num_scalar_prefetch=2,
            grid=(slots,),
            in_specs=[
                pl.BlockSpec((1, rows, rank), lambda n, i, t: (places.home_of(n, i, t), 0, 0)),
                pl.BlockSpec((1, rank, cols), lambda n, i, t: (n, 0, 0)),
            ],
            out_specs=[
                pl.BlockSpec((1, rows, rank), lambda n, i, t: (n, 0, 0)),
                pl.BlockSpec((1, rows, cols), lambda n, i, t: (n, 0, 0)),
            ],
        ),
        name="updates",
    )(ids, table, received, normed)


def send(block, shift):
    size = lax.axis_size("shard")
    if shift % size == 0:
        return block
    return lax.ppermute(block, "shard", [(s, (s + shift) % size) for s in range(size)])


def owner_exchange(stack):
    return lax.all_to_all(stack, "owner", split_axis=0, concat_axis=0, tiled=True)


def dot(a, b, contract):
    return lax.dot_general(
        a, b, (contract, ((), ())), precision=HIGH_PREC, preferred_element_type=jnp.float32
    )


TN = ((0,), (0,))


def on_device(gradient, old_basis, moment_one, moment_two, slot_expert, cost):
    slots = gradient.shape[0]
    rank, cols = moment_one.shape[1] * lax.axis_size("shard"), gradient.shape[2]
    owners, size = lax.axis_size("owner"), lax.axis_size("shard")
    owner_now, shard_now = lax.axis_index("owner"), lax.axis_index("shard")
    places = Places(owners, slots)
    ids = jnp.stack([owner_now, shard_now])
    table = slot_expert
    count = lax.dynamic_slice_in_dim(cost, owner_now * slots + shard_now, 1)

    def onward(shift, ids_ref):
        return lax.rem(ids_ref[1] + shift, size)

    outgoing = pick_stack(ids, table, old_basis, owners, places.slot_for)
    arrived = owner_exchange(outgoing)
    grad_out = pick_apart(ids, table, gradient, size, lambda k, i, t: onward(k, i))
    grads = [send(block, k) for k, block in enumerate(grad_out)]
    square = sum(dot(g, g, TN) for g in grads)
    basis_out = pick_apart(
        ids, table, arrived, size, lambda k, i, t: places.holder_of(onward(k, i), i, t)
    )
    bases = [send(block, k) for k, block in enumerate(basis_out)]
    start = sum(dot(b, g, TN) for b, g in zip(bases, grads))

    head, projected = refine(count, square, start)

    proj_rows = rank // size
    proj_out = pick_apart(
        ids,
        table,
        projected.reshape(size, proj_rows, cols),
        size,
        lambda k, i, t: lax.rem(i[1] - k + size, size),
        steps=1,
    )
    proj_home = [send(block, -k) for k, block in enumerate(proj_out)]
    proj_recv = owner_exchange(stack_for_holders(places, ids, table, proj_home, 1))
    moment_new, second_new, normed = adam(places, ids, table, proj_recv, moment_one, moment_two)
    normed_all = lax.all_gather(normed, "shard", axis=1, tiled=True)

    fresh = [jnp.where(count[0] > 0, dot(g, head, NT), b) for g, b in zip(grads, bases)]
    basis_home = [send(block, -k) for k, block in enumerate(fresh)]
    basis_recv = owner_exchange(stack_for_holders(places, ids, table, basis_home, 4))

    basis_slot, update = updates(places, ids, table, basis_recv, normed_all, slots)
    return (basis_slot, moment_new, second_new, update)


def solution(mesh):
    spec = P("owner", "shard", None)
    return jax.shard_map(
        on_device,
        mesh=mesh,
        in_specs=(spec, spec, spec, spec, P(), P()),
        out_specs=(spec, spec, spec, spec),
        check_vma=False,
    )
```
